32 devices in a mesh: row: 4 (over y, core), col: 8 (over z, x).
Axes of the slice: x: 2, y: 2, z: 4, core: 2. Of those that a mesh axis runs over, the one named last changes fastest.
Arguments:
- offsets: float32 [3, 8192], P(None, ('row', 'col')), may hold values from 0 to 11
- cells: int32 [3, 64], replicated, may hold values from 0 to 3, as said below
- types: int32 [8192], P(('row', 'col')), may hold values from 0 to 3, as said below
- mask: int32 [4, 16, 4, 16], P(None, 'col', 'row'), may hold values from 0 to 1, as said below
- chi_table: float32 [4], replicated, may hold values from 2 to 10.1
- eta_table: float32 [4], replicated, may hold values from 13 to 18
- gamma_table: float32 [4], replicated, may hold values from 0.4 to 0.8
Outputs:
- charges: float32 [8192], P(('row', 'col'))
The draws below stay inside these ranges and needn't reach their ends.
Inputs may be any that keep to these rules, and one draw needn't show every extreme that they name: The cells of the blocks are a permutation of all 4 x 4 x 4 cells: each cell holds exactly one block. The mask marks a pair of blocks exactly when their cells are equal or adjacent on the periodic grid in every dimension; it is symmetric and each block is marked with exactly 27 blocks, itself included. `types`: types 2 and 3 grow more common along the atoms, from none in the first 256 atoms to nearly all in the last.
All inputs are finite; a program needn't handle non-finite values.
Results may differ from the reference program's by a relative error of at most 0.0003.
Values sent between devices are 32-bit elements; how exact they have to be, the bound alone decides.
No kernel may reach another device: no remote copies, remote signals or barrier semaphores. Data moves between devices by JAX's collectives and lax.ppermute only.
A program may use at most 64 MiB of HBM per device.

```python
import math
import jax
import jax.numpy as jnp
from jax import lax

BLOCK = 128
BPD = 2
NTYPES = 4
NEIGHBORS = 27
GRID_Z = 4
ITERS = 3
RB = 16
NB = 64
ATOMS = 8192
SPAN = 256
GRID_X = 4
GRID_Y = 4
N_ROW = 4


def block_cells(key):
    order = jax.random.permutation(jax.random.fold_in(key, 11), NB).astype(jnp.int32)
    first = order // (GRID_Y * GRID_Z)
    second = order // GRID_Z % GRID_Y
    third = order % GRID_Z
    return jnp.stack([first, second, third], axis=0)


def draw_cells(key, part):
    return block_cells(key)


def draw_mask(key, part):
    placed = block_cells(key)
    grid = jnp.array([GRID_X, GRID_Y, GRID_Z], jnp.int32)[:, None, None]
    diff = placed[:, :, None] - placed[:, None, :]
    wrapped = (diff + grid // 2) % grid - grid // 2
    near = jnp.all(jnp.abs(wrapped) <= 1, axis=0).astype(jnp.int32)
    return near.reshape(N_ROW, RB, N_ROW, RB)


def draw_types(key, part):
    spans = NB // BPD
    owner = jnp.arange(ATOMS, dtype=jnp.int32) // SPAN
    level = jax.random.randint(jax.random.fold_in(key, 21), (ATOMS,), 0, spans)
    within = jax.random.randint(jax.random.fold_in(key, 22), (ATOMS,), 0, 2)
    return (2 * (level < owner).astype(jnp.int32) + within).astype(jnp.int32)


def draw_chi_table(key, part):
    base = 2.0 + 2.2 * jnp.arange(NTYPES, dtype=jnp.float32)
    jitter = jax.random.uniform(jax.random.fold_in(key, 31), (NTYPES,), jnp.float32, 0.0, 1.5)
    return (base + jitter).astype(jnp.float32)


def block_scale(stream_key, dims, split, low, largest):
    loudness = 1.0
    for axis_at, parts in split:
        draws = jax.random.uniform(jax.random.fold_in(jax.random.fold_in(stream_key, 6), axis_at), (parts,), jnp.float32, low / len(split), largest / len(split))
        loudness = loudness * jnp.repeat(jnp.exp(draws), dims[axis_at] // parts).reshape((-1,) + (1,) * (len(dims) - 1 - axis_at))
    return loudness


def setup_inputs(seed: int = 0) -> dict:
    key_list = jax.random.split(jax.random.key(seed), 8)
    offsets = jnp.clip(11.0 * jax.random.uniform(key_list[0], (3, ATOMS), jnp.float32) ** block_scale(key_list[0], (3, ATOMS), ((1, 32),), -0.2, 0.2), 0.0, 11.0)
    cells = draw_cells(jax.random.fold_in(key_list[7], 71), 0)
    types = draw_types(jax.random.fold_in(key_list[7], 71), 0)
    mask = draw_mask(jax.random.fold_in(key_list[7], 71), 0)
    chi_table = draw_chi_table(jax.random.fold_in(key_list[7], 71), 0)
    eta_table = jnp.clip(jax.random.uniform(key_list[5], (NTYPES,), jnp.float32, 13.0, 18.0), 13.0, 18.0)
    gamma_table = jnp.clip(jnp.exp(jax.random.uniform(key_list[6], (NTYPES,), jnp.float32, math.log(0.4), math.log(0.8))), 0.4, 0.8)
    return dict(offsets=offsets, cells=cells, types=types, mask=mask, chi_table=chi_table, eta_table=eta_table, gamma_table=gamma_table)


coulomb = 14.4
cutoff = 10.0
cell_side = 11.0
ref_group = 64

def taper(dist):
    xval = dist / cutoff
    poly = 1.0 + xval ** 4 * (-35.0 + xval * (84.0 + xval * (-70.0 + 20.0 * xval)))
    return jnp.where(xval < 1.0, poly, 0.0)

def coupling(tgt, src, tgt_cell, src_cell, same, grid):
    half = grid[:, None] // 2
    shift = ((src_cell - tgt_cell + half) % grid[:, None] - half).astype(jnp.float32) * cell_side
    radius_sq = jnp.zeros((tgt.shape[1], tgt.shape[2], src.shape[2]), jnp.float32)
    for comp in range(3):
        delta = shift[comp][:, None, None] + src[comp][:, None, :] - tgt[comp][:, :, None]
        radius_sq = radius_sq + delta * delta
    dist = jnp.sqrt(radius_sq)
    paired = tgt[3][:, :, None] * src[3][:, None, :]
    shield = 1.0 / (paired * jnp.sqrt(paired))
    kern = coulomb * taper(dist) / jnp.cbrt(radius_sq * dist + shield)
    width = tgt.shape[2]
    diag = jnp.arange(width)[:, None] == jnp.arange(width)[None, :]
    return jnp.where(same[:, None, None] & diag[None], 0.0, kern)

def pick(kinds, table):
    return lax.optimization_barrier(jnp.sum(jnp.where(kinds, table[:, None], 0.0), axis=0))

def reference(offsets, cells, types, mask, chi_table, eta_table, gamma_table):
    nblocks = cells.shape[1]
    kinds = jnp.arange(chi_table.shape[0])[:, None] == types[None, :]
    chi = pick(kinds, chi_table)
    eta = pick(kinds, eta_table)
    gamma = pick(kinds, gamma_table)
    geo = jnp.concatenate([offsets, gamma[None]], axis=0).reshape(4, nblocks, BLOCK)
    grid = jnp.array([GRID_X, GRID_Y, GRID_Z], jnp.int32)
    flat = mask.reshape(nblocks * nblocks)
    marked = jnp.sum(flat)
    groups = (nblocks * NEIGHBORS + ref_group - 1) // ref_group
    slots = jnp.nonzero(flat, size=groups * ref_group, fill_value=0)[0].astype(jnp.int32)
    block_ids = jnp.arange(nblocks, dtype=jnp.int32)

    def matvec(vec):
        spread = vec.reshape(2, nblocks, BLOCK)

        def turn(acc, step):
            picked = lax.dynamic_slice_in_dim(slots, step * ref_group, ref_group)
            live = step * ref_group + jnp.arange(ref_group) < marked
            tgt_blk = picked // nblocks
            src_blk = picked % nblocks
            kern = coupling(geo[:, tgt_blk], geo[:, src_blk], cells[:, tgt_blk], cells[:, src_blk], block_ids[tgt_blk] == block_ids[src_blk], grid)
            kern = jnp.where(live[:, None, None], kern, 0.0)
            contrib = jnp.einsum('gij,kgj->kgi', kern, spread[:, src_blk], precision=lax.Precision.HIGHEST)
            return (acc.at[:, tgt_blk].add(contrib), None)
        acc, _ = lax.scan(turn, jnp.zeros((2, nblocks, BLOCK), jnp.float32), jnp.arange(groups, dtype=jnp.int32))
        return acc.reshape(2, nblocks * BLOCK) + eta[None] * vec
    rhs = jnp.stack([-chi, -jnp.ones_like(chi)], axis=0)
    solution = jnp.zeros_like(rhs)
    residual = rhs
    direction = rhs
    norm_now = lax.optimization_barrier(jnp.sum(residual * residual, axis=1))
    for step in range(ITERS):
        image = matvec(direction)
        alpha = norm_now / lax.optimization_barrier(jnp.sum(direction * image, axis=1))
        solution = solution + alpha[:, None] * direction
        residual = residual - alpha[:, None] * image
        norm_next = lax.optimization_barrier(jnp.sum(residual * residual, axis=1))
        direction = residual + (norm_next / norm_now)[:, None] * direction
        norm_now = norm_next
    totals = lax.optimization_barrier(jnp.sum(solution, axis=1))
    return solution[0] - totals[0] / totals[1] * solution[1]
```

```python
import itertools
import jax
import jax.numpy as jnp
from jax import lax
from jax.experimental import pallas as pl
from jax.experimental.pallas import tpu as pltpu
from jax.sharding import PartitionSpec as P

BLOCK = 128
GRID_Z = 4
ITERS = 3

coulomb = 14.4
cutoff = 10.0
cell_side = 11.0
STEPS = tuple(itertools.product((-1, 0, 1), repeat=3))
SELF = STEPS.index((0, 0, 0))
AXES = ("row", "col")
F32 = jnp.float32


def column(row):
    return jnp.transpose(jnp.broadcast_to(row, (BLOCK, BLOCK)))


def lane_sums(acc):
    return jnp.sum(jnp.transpose(acc), axis=0, keepdims=True)


def pair_sums(vec):
    part = jnp.sum(vec.reshape(-1, 8, BLOCK), axis=0)
    part = jnp.broadcast_to(jnp.sum(part, axis=1, keepdims=True), (8, BLOCK))
    part = part + pltpu.roll(part, 4, 0)
    return part + pltpu.roll(part, 2, 0)


def scale(vec, factor):
    return (vec.reshape(-1, 8, BLOCK) * factor[None]).reshape(vec.shape)


def send_rows(out_ref, rows):
    own = jnp.concatenate(rows, axis=0)
    own = jnp.concatenate([own] * (8 // own.shape[0]), axis=0)
    out_ref[...] = jnp.broadcast_to(own[None], out_ref.shape)


def by_type(kinds, table_ref):
    out = jnp.full(kinds.shape, table_ref[0], F32)
    for kind in range(1, table_ref.shape[0]):
        out = jnp.where(kinds == float(kind), table_ref[kind], out)
    return out


def build_kernel(nb_ref, chi_ref, eta_ref, gamma_ref, geo_ref, h_ref, send_ref, rhs_ref,
                 shield_ref, tgt_ref, acc_ref):
    n_blk = shield_ref.shape[0]
    bpd = h_ref.shape[0] // len(STEPS)
    kinds = geo_ref[pl.ds(3, n_blk, stride=4), :]
    gamma = by_type(kinds, gamma_ref)
    shield_ref[...] = 1.0 / (gamma * jnp.sqrt(gamma))
    rhs_ref[pl.ds(0, n_blk, stride=2), :] = -by_type(kinds, chi_ref)
    rhs_ref[pl.ds(1, n_blk, stride=2), :] = jnp.full((n_blk, BLOCK), -1.0, F32)
    rows = []
    for own in range(bpd):
        mine = nb_ref[own * len(STEPS) + SELF]
        for comp in range(3):
            tgt_ref[comp] = column(geo_ref[pl.ds(4 * mine + comp, 1), :])
        tgt_ref[3] = column(shield_ref[pl.ds(mine, 1), :])
        acc_ref[...] = jnp.zeros(acc_ref.shape, F32)

        def pair(at, carry, own=own):
            blk = nb_ref[own * len(STEPS) + at]
            move = (at // 9 - 1, at // 3 % 3 - 1, at % 3 - 1)
            src = [
                geo_ref[pl.ds(4 * blk + comp, 1), :] + move[comp].astype(F32) * cell_side
                for comp in range(3)
            ]
            src = [jnp.broadcast_to(s, (8, BLOCK)) for s in src]
            shd = jnp.broadcast_to(shield_ref[pl.ds(blk, 1), :], (8, BLOCK))
            first = jnp.broadcast_to(rhs_ref[pl.ds(2 * blk, 1), :], (8, BLOCK))
            second = jnp.broadcast_to(rhs_ref[pl.ds(2 * blk + 1, 1), :], (8, BLOCK))
            for chunk in range(BLOCK // 8):
                at_rows = pl.ds(8 * chunk, 8)
                gap = [src[comp] - tgt_ref[comp, at_rows, :] for comp in range(3)]
                rsq = gap[0] * gap[0] + gap[1] * gap[1] + gap[2] * gap[2]
                dist = rsq * lax.rsqrt(jnp.maximum(rsq, 1e-30))
                left = jnp.maximum(cutoff - dist, 0.0)
                sq = left * left
                base = coulomb / cutoff**4
                poly = base + dist * (
                    4.0 * base / cutoff
                    + dist * (10.0 * base / cutoff**2 + dist * (20.0 * base / cutoff**3))
                )
                wide = rsq * dist + shd * tgt_ref[3, at_rows, :]
                kern = sq * sq * poly * jnp.exp2(jnp.log2(wide) * (-1.0 / 3.0))
                h_ref[own * len(STEPS) + at, at_rows, :] = kern
                acc_ref[0, at_rows, :] += kern * first
                acc_ref[1, at_rows, :] += kern * second
            return carry

        lax.fori_loop(0, len(STEPS), pair, 0)
        here = own * len(STEPS) + SELF
        diag = lax.broadcasted_iota(jnp.int32, (BLOCK, BLOCK), 0) == lax.broadcasted_iota(
            jnp.int32, (BLOCK, BLOCK), 1
        )
        eta = by_type(geo_ref[pl.ds(4 * mine + 3, 1), :], eta_ref)
        old = h_ref[here]
        new = jnp.where(diag, eta, old)
        h_ref[here] = new
        for k in range(2):
            fix = (new - old) * rhs_ref[pl.ds(2 * mine + k, 1), :]
            rows.append(lane_sums(acc_ref[k] + fix))
    send_rows(send_ref, rows)


def image_rows(nb_ref, h_ref, dir_ref):
    rows = []
    half = BLOCK // 2
    bpd = h_ref.shape[0] // len(STEPS)
    for own in range(bpd):
        parts = ([], [])
        for at_half in range(2):
            acc = [jnp.zeros((half, BLOCK), F32), jnp.zeros((half, BLOCK), F32)]
            for at in range(len(STEPS)):
                pair = own * len(STEPS) + at
                blk = nb_ref[pair]
                h = h_ref[pair, half * at_half : half * (at_half + 1), :]
                for k in range(2):
                    acc[k] = acc[k] + h * dir_ref[pl.ds(2 * blk + k, 1), :]
            for k in range(2):
                parts[k].append(acc[k])
        for k in range(2):
            rows.append(lane_sums(jnp.concatenate(parts[k], axis=0)))
    return rows


def step(image, res, direction, sol):
    norm = pair_sums(res * res)
    alpha = norm / pair_sums(direction * image)
    res = res - scale(image, alpha)
    ratio = pair_sums(res * res) / norm
    move = scale(direction, alpha)
    sol = move if sol is None else sol + move
    return res, res + scale(direction, ratio), sol


def first_kernel(nb_ref, h_ref, rhs_ref, image_ref, send_ref, res_ref, dir_ref, sol_ref):
    rhs = rhs_ref[...]
    res, direction, sol = step(image_ref[...], rhs, rhs, None)
    res_ref[...] = res
    dir_ref[...] = direction
    sol_ref[...] = sol
    send_rows(send_ref, image_rows(nb_ref, h_ref, dir_ref))


def later_kernel(nb_ref, h_ref, res_in, dir_in, sol_in, image_ref, send_ref, res_ref, dir_ref,
                 sol_ref):
    res, direction, sol = step(image_ref[...], res_in[...], dir_in[...], sol_in[...])
    res_ref[...] = res
    dir_ref[...] = direction
    sol_ref[...] = sol
    send_rows(send_ref, image_rows(nb_ref, h_ref, dir_ref))


def last_kernel(nb_ref, res_ref, dir_ref, sol_ref, image_ref, out_ref, full_ref):
    res = res_ref[...]
    direction = dir_ref[...]
    alpha = pair_sums(res * res) / pair_sums(direction * image_ref[...])
    sol = sol_ref[...] + scale(direction, alpha)
    full_ref[...] = sol
    totals = pair_sums(sol)
    ratio = totals[0:1] / totals[1:2]
    for own in range(out_ref.shape[0]):
        mine = nb_ref[own * len(STEPS) + SELF]
        out_ref[pl.ds(own, 1), :] = (
            full_ref[pl.ds(2 * mine, 1), :] - ratio * full_ref[pl.ds(2 * mine + 1, 1), :]
        )


def spread(buf, n_dev):
    rows = buf.reshape(-1, BLOCK)
    return lax.all_to_all(rows, AXES, 0, 0, tiled=True)


def per_device(offsets, cells, types, mask, chi_table, eta_table, gamma_table):
    n_row = lax.axis_size("row")
    n_col = lax.axis_size("col")
    n_dev = n_row * n_col
    me = lax.axis_index("row") * n_col + lax.axis_index("col")
    bpd = types.shape[0] // BLOCK
    n_blk = n_dev * bpd
    n_pair = bpd * len(STEPS)
    grid = jnp.array([n_row, n_col * bpd // GRID_Z, GRID_Z], jnp.int32)[:, None]

    mine = lax.dynamic_slice_in_dim(cells, me * bpd, bpd, axis=1)
    moves = jnp.array(STEPS, jnp.int32).T
    near = ((mine[:, :, None] + moves[:, None, :] + grid[:, :, None]) % grid[:, :, None])
    found = jnp.all(near.reshape(3, n_pair, 1) == cells[:, None, :], axis=0)
    nb = jnp.sum(jnp.where(found, jnp.arange(n_blk, dtype=jnp.int32)[None], 0), axis=1)

    geo = jnp.concatenate([offsets, types.astype(F32)[None]], axis=0)
    geo = geo.reshape(4, bpd, BLOCK).transpose(1, 0, 2).reshape(1, 4 * bpd, BLOCK)
    geo = spread(jnp.broadcast_to(geo, (n_dev, 4 * bpd, BLOCK)), n_dev)

    smem = pl.BlockSpec(memory_space=pltpu.SMEM)
    vmem = pl.BlockSpec(memory_space=pltpu.VMEM)
    n_vec = 2 * n_blk
    full = jax.ShapeDtypeStruct((n_vec, BLOCK), F32)
    send = jax.ShapeDtypeStruct((n_vec // 8, 8, BLOCK), F32)
    matrix, image, rhs = pl.pallas_call(
        build_kernel,
        out_shape=(pltpu.VMEM((n_pair, BLOCK, BLOCK), F32), send, full),
        in_specs=[smem] * 4 + [vmem],
        out_specs=(vmem,) * 3,
        scratch_shapes=[
            pltpu.VMEM((n_blk, BLOCK), F32),
            pltpu.VMEM((4, BLOCK, BLOCK), F32),
            pltpu.VMEM((2, BLOCK, BLOCK), F32),
        ],
        name="build",
    )(nb, chi_table, eta_table, gamma_table, geo)
    image = spread(image, n_dev)
    image, res, direction, sol = pl.pallas_call(
        first_kernel,
        out_shape=(send, full, full, full),
        in_specs=[smem] + [vmem] * 3,
        out_specs=(vmem,) * 4,
        name="first",
    )(nb, matrix, rhs, image)
    image = spread(image, n_dev)
    for _ in range(ITERS - 2):
        image, res, direction, sol = pl.pallas_call(
            later_kernel,
            out_shape=(send, full, full, full),
            in_specs=[smem] + [vmem] * 5,
            out_specs=(vmem,) * 4,
            name="later",
        )(nb, matrix, res, direction, sol, image)
        image = spread(image, n_dev)
    out = pl.pallas_call(
        last_kernel,
        out_shape=jax.ShapeDtypeStruct((bpd, BLOCK), F32),
        in_specs=[smem] + [vmem] * 4,
        out_specs=vmem,
        scratch_shapes=[pltpu.VMEM((n_vec, BLOCK), F32)],
        name="last",
    )(nb, res, direction, sol, image)
    return out.reshape(bpd * BLOCK)


def solution(mesh):
    placed = (
        P(None, AXES),
        P(),
        P(AXES),
        P(None, "col", "row", None),
        P(),
        P(),
        P(),
    )
    return jax.shard_map(
        per_device, mesh=mesh, in_specs=placed, out_specs=P(AXES), check_vma=False
    )
```

```python
import itertools
import jax
import jax.numpy as jnp
from jax import lax
from jax.experimental import pallas as pl
from jax.experimental.pallas import tpu as pltpu
from jax.sharding import PartitionSpec as P

BLOCK = 128
GRID_Z = 4
ITERS = 3

coulomb = 14.4
cutoff = 10.0
cell_side = 11.0
STEPS = tuple(itertools.product((-1, 0, 1), repeat=3))
SELF = STEPS.index((0, 0, 0))
AXES = ("row", "col")
F32 = jnp.float32


def column(row):
    return jnp.transpose(jnp.broadcast_to(row, (BLOCK, BLOCK)))


def lane_sums(acc):
    return jnp.sum(jnp.transpose(acc), axis=0, keepdims=True)


def pair_sums(vec):
    part = jnp.sum(vec.reshape(-1, 8, BLOCK), axis=0)
    part = jnp.broadcast_to(jnp.sum(part, axis=1, keepdims=True), (8, BLOCK))
    part = part + pltpu.roll(part, 4, 0)
    return part + pltpu.roll(part, 2, 0)


def scale(vec, factor):
    return (vec.reshape(-1, 8, BLOCK) * factor[None]).reshape(vec.shape)


def send_rows(out_ref, rows):
    own = jnp.concatenate(rows, axis=0)
    own = jnp.concatenate([own] * (8 // own.shape[0]), axis=0)
    out_ref[...] = jnp.broadcast_to(own[None], out_ref.shape)


def by_type(kinds, table_ref):
    out = jnp.full(kinds.shape, table_ref[0], F32)
    for kind in range(1, table_ref.shape[0]):
        out = jnp.where(kinds == float(kind), table_ref[kind], out)
    return out


def build_kernel(nb_ref, chi_ref, eta_ref, gamma_ref, geo_ref, h_ref, send_ref, rhs_ref,
                 shield_ref, tgt_ref, acc_ref):
    n_blk = shield_ref.shape[0]
    bpd = h_ref.shape[0] // len(STEPS)
    kinds = geo_ref[pl.ds(3, n_blk, stride=4), :]
    gamma = by_type(kinds, gamma_ref)
    shield_ref[...] = 1.0 / (gamma * jnp.sqrt(gamma))
    rhs_ref[pl.ds(0, n_blk, stride=2), :] = -by_type(kinds, chi_ref)
    rhs_ref[pl.ds(1, n_blk, stride=2), :] = jnp.full((n_blk, BLOCK), -1.0, F32)
    rows = []
    for own in range(bpd):
        mine = nb_ref[own * len(STEPS) + SELF]
        for comp in range(3):
            tgt_ref[comp] = column(geo_ref[pl.ds(4 * mine + comp, 1), :])
        tgt_ref[3] = column(shield_ref[pl.ds(mine, 1), :])
        acc_ref[...] = jnp.zeros(acc_ref.shape, F32)

        def pair(at, carry, own=own):
            blk = nb_ref[own * len(STEPS) + at]
            move = (at // 9 - 1, at // 3 % 3 - 1, at % 3 - 1)
            src = [
                geo_ref[pl.ds(4 * blk + comp, 1), :] + move[comp].astype(F32) * cell_side
                for comp in range(3)
            ]
            src = [jnp.broadcast_to(s, (8, BLOCK)) for s in src]
            shd = jnp.broadcast_to(shield_ref[pl.ds(blk, 1), :], (8, BLOCK))
            first = jnp.broadcast_to(rhs_ref[pl.ds(2 * blk, 1), :], (8, BLOCK))
            second = jnp.broadcast_to(rhs_ref[pl.ds(2 * blk + 1, 1), :], (8, BLOCK))
            for chunk in range(BLOCK // 8):
                at_rows = pl.ds(8 * chunk, 8)
                gap = [src[comp] - tgt_ref[comp, at_rows, :] for comp in range(3)]
                rsq = gap[0] * gap[0] + gap[1] * gap[1] + gap[2] * gap[2]
                dist = rsq * lax.rsqrt(jnp.maximum(rsq, 1e-30))
                left = jnp.maximum(cutoff - dist, 0.0)
                sq = left * left
                base = coulomb / cutoff**4
                poly = base + dist * (
                    4.0 * base / cutoff
                    + dist * (10.0 * base / cutoff**2 + dist * (20.0 * base / cutoff**3))
                )
                wide = rsq * dist + shd * tgt_ref[3, at_rows, :]
                kern = sq * sq * poly * jnp.exp2(jnp.log2(wide) * (-1.0 / 3.0))
                h_ref[own * len(STEPS) + at, at_rows, :] = kern
                acc_ref[0, at_rows, :] += kern * first
                acc_ref[1, at_rows, :] += kern * second
            return carry

        lax.fori_loop(0, len(STEPS), pair, 0)
        here = own * len(STEPS) + SELF
        diag = lax.broadcasted_iota(jnp.int32, (BLOCK, BLOCK), 0) == lax.broadcasted_iota(
            jnp.int32, (BLOCK, BLOCK), 1
        )
        eta = by_type(geo_ref[pl.ds(4 * mine + 3, 1), :], eta_ref)
        old = h_ref[here]
        new = jnp.where(diag, eta, old)
        h_ref[here] = new
        for k in range(2):
            fix = (new - old) * rhs_ref[pl.ds(2 * mine + k, 1), :]
            rows.append(lane_sums(acc_ref[k] + fix))
    send_rows(send_ref, rows)


def image_rows(nb_ref, h_ref, dir_ref):
    rows = []
    half = BLOCK // 2
    bpd = h_ref.shape[0] // len(STEPS)
    for own in range(bpd):
        parts = ([], [])
        for at_half in range(2):
            acc = [jnp.zeros((half, BLOCK), F32), jnp.zeros((half, BLOCK), F32)]
            for at in range(len(STEPS)):
                pair = own * len(STEPS) + at
                blk = nb_ref[pair]
                h = h_ref[pair, half * at_half : half * (at_half + 1), :]
                for k in range(2):
                    acc[k] = acc[k] + h * dir_ref[pl.ds(2 * blk + k, 1), :]
            for k in range(2):
                parts[k].append(acc[k])
        for k in range(2):
            rows.append(lane_sums(jnp.concatenate(parts[k], axis=0)))
    return rows


def step(image, res, direction, sol):
    norm = pair_sums(res * res)
    alpha = norm / pair_sums(direction * image)
    res = res - scale(image, alpha)
    ratio = pair_sums(res * res) / norm
    move = scale(direction, alpha)
    sol = move if sol is None else sol + move
    return res, res + scale(direction, ratio), sol


def first_kernel(nb_ref, h_ref, rhs_ref, image_ref, send_ref, res_ref, dir_ref, sol_ref):
    rhs = rhs_ref[...]
    res, direction, sol = step(image_ref[...], rhs, rhs, None)
    res_ref[...] = res
    dir_ref[...] = direction
    sol_ref[...] = sol
    send_rows(send_ref, image_rows(nb_ref, h_ref, dir_ref))


def later_kernel(nb_ref, h_ref, res_in, dir_in, sol_in, image_ref, send_ref, res_ref, dir_ref,
                 sol_ref):
    res, direction, sol = step(image_ref[...], res_in[...], dir_in[...], sol_in[...])
    res_ref[...] = res
    dir_ref[...] = direction
    sol_ref[...] = sol
    send_rows(send_ref, image_rows(nb_ref, h_ref, dir_ref))


def last_kernel(nb_ref, res_ref, dir_ref, sol_ref, image_ref, out_ref, full_ref):
    res = res_ref[...]
    direction = dir_ref[...]
    alpha = pair_sums(res * res) / pair_sums(direction * image_ref[...])
    sol = sol_ref[...] + scale(direction, alpha)
    full_ref[...] = sol
    totals = pair_sums(sol)
    ratio = totals[0:1] / totals[1:2]
    for own in range(out_ref.shape[0]):
        mine = nb_ref[own * len(STEPS) + SELF]
        out_ref[pl.ds(own, 1), :] = (
            full_ref[pl.ds(2 * mine, 1), :] - ratio * full_ref[pl.ds(2 * mine + 1, 1), :]
        )


def keep(*arrays):
    return [pltpu.with_memory_space_constraint(a, pltpu.VMEM) for a in arrays]


def spread(buf):
    rows = buf.reshape(-1, BLOCK)
    return lax.all_to_all(rows, AXES, 0, 0, tiled=True)


def per_device(offsets, cells, types, mask, chi_table, eta_table, gamma_table):
    n_row = lax.axis_size("row")
    n_col = lax.axis_size("col")
    n_dev = n_row * n_col
    me = lax.axis_index("row") * n_col + lax.axis_index("col")
    bpd = types.shape[0] // BLOCK
    n_blk = n_dev * bpd
    n_pair = bpd * len(STEPS)
    grid = jnp.array([n_row, n_col * bpd // GRID_Z, GRID_Z], jnp.int32)[:, None]

    mine = lax.dynamic_slice_in_dim(cells, me * bpd, bpd, axis=1)
    moves = jnp.array(STEPS, jnp.int32).T
    near = ((mine[:, :, None] + moves[:, None, :] + grid[:, :, None]) % grid[:, :, None])
    found = jnp.all(near.reshape(3, n_pair, 1) == cells[:, None, :], axis=0)
    nb = jnp.sum(jnp.where(found, jnp.arange(n_blk, dtype=jnp.int32)[None], 0), axis=1)

    geo = jnp.concatenate([offsets, types.astype(F32)[None]], axis=0)
    geo = geo.reshape(4, bpd, BLOCK).transpose(1, 0, 2).reshape(1, 4 * bpd, BLOCK)
    geo = spread(jnp.broadcast_to(geo, (n_dev, 4 * bpd, BLOCK)))

    smem = pl.BlockSpec(memory_space=pltpu.SMEM)
    vmem = pl.BlockSpec(memory_space=pltpu.VMEM)
    params = pltpu.CompilerParams(vmem_limit_bytes=24 * 2**20)
    n_vec = 2 * n_blk
    full = pltpu.VMEM((n_vec, BLOCK), F32)
    send = pltpu.VMEM((n_vec // 8, 8, BLOCK), F32)
    matrix, image, rhs = pl.pallas_call(
        build_kernel,
        out_shape=(pltpu.VMEM((n_pair, BLOCK, BLOCK), F32), send, full),
        in_specs=[smem] * 4 + [vmem],
        out_specs=(vmem,) * 3,
        scratch_shapes=[
            pltpu.VMEM((n_blk, BLOCK), F32),
            pltpu.VMEM((4, BLOCK, BLOCK), F32),
            pltpu.VMEM((2, BLOCK, BLOCK), F32),
        ],
        compiler_params=params,
        name="build",
    )(nb, chi_table, eta_table, gamma_table, *keep(geo))
    image = spread(image)
    image, res, direction, sol = pl.pallas_call(
        first_kernel,
        out_shape=(send, full, full, full),
        in_specs=[smem] + [vmem] * 3,
        out_specs=(vmem,) * 4,
        compiler_params=params,
        name="first",
    )(nb, *keep(matrix, rhs, image))
    image = spread(image)
    for _ in range(ITERS - 2):
        image, res, direction, sol = pl.pallas_call(
            later_kernel,
            out_shape=(send, full, full, full),
            in_specs=[smem] + [vmem] * 5,
            out_specs=(vmem,) * 4,
            compiler_params=params,
            name="later",
        )(nb, *keep(matrix, res, direction, sol, image))
        image = spread(image)
    out = pl.pallas_call(
        last_kernel,
        out_shape=jax.ShapeDtypeStruct((bpd, BLOCK), F32),
        in_specs=[smem] + [vmem] * 4,
        out_specs=vmem,
        scratch_shapes=[pltpu.VMEM((n_vec, BLOCK), F32)],
        compiler_params=params,
        name="last",
    )(nb, *keep(res, direction, sol, image))
    return out.reshape(bpd * BLOCK)


def solution(mesh):
    placed = (
        P(None, AXES),
        P(),
        P(AXES),
        P(None, "col", "row", None),
        P(),
        P(),
        P(),
    )
    return jax.shard_map(
        per_device, mesh=mesh, in_specs=placed, out_specs=P(AXES), check_vma=False
    )
```

```python
import itertools
import jax
import jax.numpy as jnp
from jax import lax
from jax.experimental import pallas as pl
from jax.experimental.pallas import tpu as pltpu
from jax.sharding import PartitionSpec as P

BLOCK = 128
GRID_Z = 4
ITERS = 3

coulomb = 14.4
cutoff = 10.0
cell_side = 11.0
unit = (20.0 * coulomb / cutoff**7) ** (1.0 / 6.0)
reach = unit * cutoff
STEPS = tuple(itertools.product((-1, 0, 1), repeat=3))
SELF = STEPS.index((0, 0, 0))
AXES = ("row", "col")
F32 = jnp.float32


def column(row):
    return jnp.transpose(jnp.broadcast_to(row, (BLOCK, BLOCK)))


def lane_sums(acc):
    return jnp.sum(jnp.transpose(acc), axis=0, keepdims=True)


def pair_sums(vec):
    part = jnp.sum(vec.reshape(-1, 8, BLOCK), axis=0)
    part = jnp.broadcast_to(jnp.sum(part, axis=1, keepdims=True), (8, BLOCK))
    part = part + pltpu.roll(part, 4, 0)
    return part + pltpu.roll(part, 2, 0)


def scale(vec, factor):
    return (vec.reshape(-1, 8, BLOCK) * factor[None]).reshape(vec.shape)


def send_rows(out_ref, rows):
    own = jnp.concatenate(rows, axis=0)
    own = jnp.concatenate([own] * (8 // own.shape[0]), axis=0)
    out_ref[...] = jnp.broadcast_to(own[None], out_ref.shape)


def by_type(kinds, table_ref, which):
    n_kind = table_ref.shape[0] // 3
    out = jnp.full(kinds.shape, table_ref[which * n_kind], F32)
    for kind in range(1, n_kind):
        out = jnp.where(kinds == float(kind), table_ref[which * n_kind + kind], out)
    return out


def pack_kernel(offsets_in, types_in, send_ref, offsets_ref, types_ref, sems):
    copies = [
        pltpu.make_async_copy(offsets_in, offsets_ref, sems.at[0]),
        pltpu.make_async_copy(types_in, types_ref, sems.at[1]),
    ]
    for copy in copies:
        copy.start()
    for copy in copies:
        copy.wait()
    rows = []
    for own in range(types_ref.shape[0]):
        at = pl.ds(own * BLOCK, BLOCK)
        rows.append(offsets_ref[:, at])
        rows.append(types_ref[pl.ds(own, 1), :].astype(F32))
    send_rows(send_ref, rows)


def build_kernel(nb_ref, table_ref, geo_ref, h_ref, send_ref, rhs_ref,
                 shield_ref, tgt_ref, acc_ref):
    n_blk = shield_ref.shape[0]
    bpd = h_ref.shape[0] // len(STEPS)
    kinds = geo_ref[pl.ds(3, n_blk, stride=4), :]
    gamma = by_type(kinds, table_ref, 2)
    shield_ref[...] = unit**1.5 / (gamma * jnp.sqrt(gamma))
    rhs_ref[pl.ds(0, n_blk, stride=2), :] = -by_type(kinds, table_ref, 0)
    rhs_ref[pl.ds(1, n_blk, stride=2), :] = jnp.full((n_blk, BLOCK), -1.0, F32)
    rows = []
    for own in range(bpd):
        mine = nb_ref[own * len(STEPS) + SELF]
        for comp in range(3):
            tgt_ref[comp] = column(geo_ref[pl.ds(4 * mine + comp, 1), :] * unit)
        tgt_ref[3] = column(shield_ref[pl.ds(mine, 1), :])
        acc_ref[...] = jnp.zeros(acc_ref.shape, F32)

        def three(at, move, own=own):
            src, shd, first = [], [], []
            for last in range(3):
                blk = nb_ref[own * len(STEPS) + 3 * at + last]
                shift = (move[0], move[1], float(last - 1) * (cell_side * unit))
                src.append([
                    jnp.broadcast_to(
                        geo_ref[pl.ds(4 * blk + comp, 1), :] * unit + shift[comp], (8, BLOCK)
                    )
                    for comp in range(3)
                ])
                shd.append(jnp.broadcast_to(shield_ref[pl.ds(blk, 1), :], (8, BLOCK)))
                first.append(jnp.broadcast_to(rhs_ref[pl.ds(2 * blk, 1), :], (8, BLOCK)))
            for chunk in range(BLOCK // 8):
                at_rows = pl.ds(8 * chunk, 8)
                tgt = [tgt_ref[comp, at_rows, :] for comp in range(4)]
                sums = [None, None]
                for last in range(3):
                    gap = [src[last][comp] - tgt[comp] for comp in range(3)]
                    rsq = gap[0] * gap[0] + gap[1] * gap[1] + gap[2] * gap[2]
                    dist = rsq * lax.rsqrt(jnp.maximum(rsq, 1e-30))
                    left = jnp.maximum(reach - dist, 0.0)
                    sq = left * left
                    poly = ((dist + 0.5 * reach) * dist + 0.2 * reach**2) * dist + 0.05 * reach**3
                    wide = rsq * dist + shd[last] * tgt[3]
                    kern = sq * sq * poly * jnp.exp2(jnp.log2(wide) * (-1.0 / 3.0))
                    h_ref[own * len(STEPS) + 3 * at + last, at_rows, :] = kern
                    part = kern * first[last]
                    sums = [part, kern] if last == 0 else [sums[0] + part, sums[1] + kern]
                acc_ref[0, at_rows, :] += sums[0]
                acc_ref[1, at_rows, :] -= sums[1]
            wrap = move[1] > 0.5 * cell_side * unit
            return (
                jnp.where(wrap, move[0] + cell_side * unit, move[0]),
                jnp.where(wrap, -cell_side * unit, move[1] + cell_side * unit),
            )

        start = jnp.float32(-cell_side * unit)
        lax.fori_loop(0, len(STEPS) // 3, three, (start, start))
        here = own * len(STEPS) + SELF
        diag = lax.broadcasted_iota(jnp.int32, (BLOCK, BLOCK), 0) == lax.broadcasted_iota(
            jnp.int32, (BLOCK, BLOCK), 1
        )
        eta = by_type(geo_ref[pl.ds(4 * mine + 3, 1), :], table_ref, 1)
        old = h_ref[here]
        new = jnp.where(diag, eta, old)
        h_ref[here] = new
        for k in range(2):
            fix = (new - old) * rhs_ref[pl.ds(2 * mine + k, 1), :]
            rows.append(lane_sums(acc_ref[k] + fix))
    send_rows(send_ref, rows)


def image_rows(nb_ref, h_ref, dir_ref):
    rows = []
    half = BLOCK // 2
    bpd = h_ref.shape[0] // len(STEPS)
    for own in range(bpd):
        parts = ([], [])
        for at_half in range(2):
            acc = [jnp.zeros((half, BLOCK), F32), jnp.zeros((half, BLOCK), F32)]
            for at in range(len(STEPS)):
                pair = own * len(STEPS) + at
                blk = nb_ref[pair]
                h = h_ref[pair, half * at_half : half * (at_half + 1), :]
                for k in range(2):
                    acc[k] = acc[k] + h * dir_ref[pl.ds(2 * blk + k, 1), :]
            for k in range(2):
                parts[k].append(acc[k])
        for k in range(2):
            rows.append(lane_sums(jnp.concatenate(parts[k], axis=0)))
    return rows


def step(image, res, direction, sol):
    norm = pair_sums(res * res)
    alpha = norm / pair_sums(direction * image)
    res = res - scale(image, alpha)
    ratio = pair_sums(res * res) / norm
    move = scale(direction, alpha)
    sol = move if sol is None else sol + move
    return res, res + scale(direction, ratio), sol


def first_kernel(nb_ref, h_ref, rhs_ref, image_ref, send_ref, res_ref, dir_ref, sol_ref):
    rhs = rhs_ref[...]
    res, direction, sol = step(image_ref[...], rhs, rhs, None)
    res_ref[...] = res
    dir_ref[...] = direction
    sol_ref[...] = sol
    send_rows(send_ref, image_rows(nb_ref, h_ref, dir_ref))


def later_kernel(nb_ref, h_ref, res_in, dir_in, sol_in, image_ref, send_ref, res_ref, dir_ref,
                 sol_ref):
    res, direction, sol = step(image_ref[...], res_in[...], dir_in[...], sol_in[...])
    res_ref[...] = res
    dir_ref[...] = direction
    sol_ref[...] = sol
    send_rows(send_ref, image_rows(nb_ref, h_ref, dir_ref))


def last_kernel(nb_ref, res_ref, dir_ref, sol_ref, image_ref, out_ref, full_ref):
    res = res_ref[...]
    direction = dir_ref[...]
    alpha = pair_sums(res * res) / pair_sums(direction * image_ref[...])
    sol = sol_ref[...] + scale(direction, alpha)
    full_ref[...] = sol
    totals = pair_sums(sol)
    ratio = totals[0:1] / totals[1:2]
    for own in range(out_ref.shape[0]):
        mine = nb_ref[own * len(STEPS) + SELF]
        out_ref[pl.ds(own, 1), :] = (
            full_ref[pl.ds(2 * mine, 1), :] - ratio * full_ref[pl.ds(2 * mine + 1, 1), :]
        )


def keep(*arrays):
    return [pltpu.with_memory_space_constraint(a, pltpu.VMEM) for a in arrays]


def spread(buf):
    rows = buf.reshape(-1, BLOCK)
    return lax.all_to_all(rows, AXES, 0, 0, tiled=True)


def per_device(offsets, cells, types, mask, chi_table, eta_table, gamma_table):
    n_row = lax.axis_size("row")
    n_col = lax.axis_size("col")
    n_dev = n_row * n_col
    me = lax.axis_index("row") * n_col + lax.axis_index("col")
    bpd = types.shape[0] // BLOCK
    n_blk = n_dev * bpd
    n_pair = bpd * len(STEPS)
    grid = jnp.array([n_row, n_col * bpd // GRID_Z, GRID_Z], jnp.int32)[:, None]

    mine = lax.dynamic_slice_in_dim(cells, me * bpd, bpd, axis=1)
    moves = jnp.array(STEPS, jnp.int32).T
    near = ((mine[:, :, None] + moves[:, None, :] + grid[:, :, None]) % grid[:, :, None])
    found = jnp.all(near.reshape(3, n_pair, 1) == cells[:, None, :], axis=0)
    nb = jnp.sum(jnp.where(found, jnp.arange(n_blk, dtype=jnp.int32)[None], 0), axis=1)

    smem = pl.BlockSpec(memory_space=pltpu.SMEM)
    vmem = pl.BlockSpec(memory_space=pltpu.VMEM)
    params = pltpu.CompilerParams(vmem_limit_bytes=24 * 2**20)
    n_vec = 2 * n_blk
    full = pltpu.VMEM((n_vec, BLOCK), F32)
    send = pltpu.VMEM((n_vec // 8, 8, BLOCK), F32)
    (geo,) = pl.pallas_call(
        pack_kernel,
        out_shape=(pltpu.VMEM((4 * n_blk // 8, 8, BLOCK), F32),),
        in_specs=[pl.BlockSpec(memory_space=pltpu.HBM)] * 2,
        out_specs=(vmem,),
        scratch_shapes=[
            pltpu.VMEM(offsets.shape, F32),
            pltpu.VMEM((bpd, BLOCK), jnp.int32),
            pltpu.SemaphoreType.DMA((2,)),
        ],
        compiler_params=params,
        name="pack",
    )(offsets, types.reshape(bpd, BLOCK))
    geo = spread(geo)
    tables = jnp.concatenate([chi_table, eta_table, gamma_table])
    matrix, image, rhs = pl.pallas_call(
        build_kernel,
        out_shape=(pltpu.VMEM((n_pair, BLOCK, BLOCK), F32), send, full),
        in_specs=[smem] * 2 + [vmem],
        out_specs=(vmem,) * 3,
        scratch_shapes=[
            pltpu.VMEM((n_blk, BLOCK), F32),
            pltpu.VMEM((4, BLOCK, BLOCK), F32),
            pltpu.VMEM((2, BLOCK, BLOCK), F32),
        ],
        compiler_params=params,
        name="build",
    )(nb, tables, *keep(geo))
    image = spread(image)
    image, res, direction, sol = pl.pallas_call(
        first_kernel,
        out_shape=(send, full, full, full),
        in_specs=[smem] + [vmem] * 3,
        out_specs=(vmem,) * 4,
        compiler_params=params,
        name="first",
    )(nb, *keep(matrix, rhs, image))
    image = spread(image)
    for _ in range(ITERS - 2):
        image, res, direction, sol = pl.pallas_call(
            later_kernel,
            out_shape=(send, full, full, full),
            in_specs=[smem] + [vmem] * 5,
            out_specs=(vmem,) * 4,
            compiler_params=params,
            name="later",
        )(nb, *keep(matrix, res, direction, sol, image))
        image = spread(image)
    out = pl.pallas_call(
        last_kernel,
        out_shape=jax.ShapeDtypeStruct((bpd, BLOCK), F32),
        in_specs=[smem] + [vmem] * 4,
        out_specs=vmem,
        scratch_shapes=[pltpu.VMEM((n_vec, BLOCK), F32)],
        compiler_params=params,
        name="last",
    )(nb, *keep(res, direction, sol, image))
    return out.reshape(bpd * BLOCK)


def solution(mesh):
    placed = (
        P(None, AXES),
        P(),
        P(AXES),
        P(None, "col", "row", None),
        P(),
        P(),
        P(),
    )
    return jax.shard_map(
        per_device, mesh=mesh, in_specs=placed, out_specs=P(AXES), check_vma=False
    )
```

```python
import itertools
import jax
import jax.numpy as jnp
from jax import lax
from jax.experimental import pallas as pl
from jax.experimental.pallas import tpu as pltpu
from jax.sharding import PartitionSpec as P

BLOCK = 128
GRID_Z = 4
ITERS = 3

coulomb = 14.4
cutoff = 10.0
cell_side = 11.0
unit = (20.0 * coulomb / cutoff**7) ** (1.0 / 6.0)
reach = unit * cutoff
STEPS = tuple(itertools.product((-1, 0, 1), repeat=3))
SELF = STEPS.index((0, 0, 0))
AXES = ("row", "col")
F32 = jnp.float32


def column(row):
    return jnp.transpose(jnp.broadcast_to(row, (BLOCK, BLOCK)))


def lane_sums(acc):
    return jnp.sum(jnp.transpose(acc), axis=0, keepdims=True)


def pair_sums(vec):
    part = jnp.sum(vec.reshape(-1, 8, BLOCK), axis=0)
    part = jnp.broadcast_to(jnp.sum(part, axis=1, keepdims=True), (8, BLOCK))
    part = part + pltpu.roll(part, 4, 0)
    return part + pltpu.roll(part, 2, 0)


def scale(vec, factor):
    return (vec.reshape(-1, 8, BLOCK) * factor[None]).reshape(vec.shape)


def send_rows(out_ref, rows):
    own = jnp.concatenate(rows, axis=0)
    own = jnp.concatenate([own] * (8 // own.shape[0]), axis=0)
    out_ref[...] = jnp.broadcast_to(own[None], out_ref.shape)


def by_type(kinds, table_ref, which):
    n_kind = table_ref.shape[0] // 3
    out = jnp.full(kinds.shape, table_ref[which * n_kind], F32)
    for kind in range(1, n_kind):
        out = jnp.where(kinds == float(kind), table_ref[which * n_kind + kind], out)
    return out


def pack_kernel(offsets_in, types_in, send_ref, offsets_ref, types_ref, sems):
    copies = [
        pltpu.make_async_copy(offsets_in, offsets_ref, sems.at[0]),
        pltpu.make_async_copy(types_in, types_ref, sems.at[1]),
    ]
    for copy in copies:
        copy.start()
    for copy in copies:
        copy.wait()
    rows = []
    for own in range(types_ref.shape[0]):
        at = pl.ds(own * BLOCK, BLOCK)
        rows.append(offsets_ref[:, at])
        rows.append(types_ref[pl.ds(own, 1), :].astype(F32))
    send_rows(send_ref, rows)


def build_kernel(nb_ref, table_ref, geo_ref, h_ref, send_ref, rhs_ref,
                 shield_ref, tgt_ref, acc_ref):
    n_blk = shield_ref.shape[0]
    bpd = h_ref.shape[0] // len(STEPS)
    kinds = geo_ref[pl.ds(3, n_blk, stride=4), :]
    gamma = by_type(kinds, table_ref, 2)
    shield_ref[...] = unit**1.5 / (gamma * jnp.sqrt(gamma))
    rhs_ref[pl.ds(0, n_blk, stride=2), :] = -by_type(kinds, table_ref, 0)
    rhs_ref[pl.ds(1, n_blk, stride=2), :] = jnp.full((n_blk, BLOCK), -1.0, F32)
    rows = []
    for own in range(bpd):
        mine = nb_ref[own * len(STEPS) + SELF]
        for comp in range(3):
            tgt_ref[comp] = column(geo_ref[pl.ds(4 * mine + comp, 1), :] * unit)
        tgt_ref[3] = column(shield_ref[pl.ds(mine, 1), :])
        acc_ref[...] = jnp.zeros(acc_ref.shape, F32)

        def three(at, move, own=own):
            src, shd, first = [], [], []
            for last in range(3):
                blk = nb_ref[own * len(STEPS) + 3 * at + last]
                shift = (move[0], move[1], float(last - 1) * (cell_side * unit))
                src.append([
                    jnp.broadcast_to(
                        geo_ref[pl.ds(4 * blk + comp, 1), :] * unit + shift[comp], (8, BLOCK)
                    )
                    for comp in range(3)
                ])
                shd.append(jnp.broadcast_to(shield_ref[pl.ds(blk, 1), :], (8, BLOCK)))
                first.append(jnp.broadcast_to(rhs_ref[pl.ds(2 * blk, 1), :], (8, BLOCK)))
            for chunk in range(BLOCK // 8):
                at_rows = pl.ds(8 * chunk, 8)
                tgt = [tgt_ref[comp, at_rows, :] for comp in range(4)]
                sums = [None, None]
                for last in range(3):
                    gap = [src[last][comp] - tgt[comp] for comp in range(3)]
                    rsq = gap[0] * gap[0] + gap[1] * gap[1] + gap[2] * gap[2]
                    dist = rsq * lax.rsqrt(jnp.maximum(rsq, 1e-30))
                    left = jnp.maximum(reach - dist, 0.0)
                    sq = left * left
                    poly = ((dist + 0.5 * reach) * dist + 0.2 * reach**2) * dist + 0.05 * reach**3
                    wide = rsq * dist + shd[last] * tgt[3]
                    kern = sq * sq * poly * jnp.exp2(jnp.log2(wide) * (-1.0 / 3.0))
                    h_ref[own * len(STEPS) + 3 * at + last, at_rows, :] = kern
                    part = kern * first[last]
                    sums = [part, kern] if last == 0 else [sums[0] + part, sums[1] + kern]
                acc_ref[0, at_rows, :] += sums[0]
                acc_ref[1, at_rows, :] -= sums[1]
            wrap = move[1] > 0.5 * cell_side * unit
            return (
                jnp.where(wrap, move[0] + cell_side * unit, move[0]),
                jnp.where(wrap, -cell_side * unit, move[1] + cell_side * unit),
            )

        start = jnp.float32(-cell_side * unit)
        lax.fori_loop(0, len(STEPS) // 3, three, (start, start))
        here = own * len(STEPS) + SELF
        diag = lax.broadcasted_iota(jnp.int32, (BLOCK, BLOCK), 0) == lax.broadcasted_iota(
            jnp.int32, (BLOCK, BLOCK), 1
        )
        eta = by_type(geo_ref[pl.ds(4 * mine + 3, 1), :], table_ref, 1)
        old = h_ref[here]
        new = jnp.where(diag, eta, old)
        h_ref[here] = new
        for k in range(2):
            fix = (new - old) * rhs_ref[pl.ds(2 * mine + k, 1), :]
            rows.append(lane_sums(acc_ref[k] + fix))
    send_rows(send_ref, rows)


def image_rows(nb_ref, h_ref, dir_ref):
    rows = []
    half = BLOCK // 2
    bpd = h_ref.shape[0] // len(STEPS)
    for own in range(bpd):
        parts = ([], [])
        for at_half in range(2):
            acc = [jnp.zeros((half, BLOCK), F32), jnp.zeros((half, BLOCK), F32)]
            for at in range(len(STEPS)):
                pair = own * len(STEPS) + at
                blk = nb_ref[pair]
                h = h_ref[pair, half * at_half : half * (at_half + 1), :]
                for k in range(2):
                    acc[k] = acc[k] + h * dir_ref[pl.ds(2 * blk + k, 1), :]
            for k in range(2):
                parts[k].append(acc[k])
        for k in range(2):
            rows.append(lane_sums(jnp.concatenate(parts[k], axis=0)))
    return rows


def step(image, res, direction, sol):
    norm = pair_sums(res * res)
    alpha = norm / pair_sums(direction * image)
    res = res - scale(image, alpha)
    ratio = pair_sums(res * res) / norm
    move = scale(direction, alpha)
    sol = move if sol is None else sol + move
    return res, res + scale(direction, ratio), sol


def first_kernel(nb_ref, h_ref, rhs_ref, image_ref, send_ref, res_ref, dir_ref, sol_ref):
    rhs = rhs_ref[...]
    res, direction, sol = step(image_ref[...], rhs, rhs, None)
    res_ref[...] = res
    dir_ref[...] = direction
    sol_ref[...] = sol
    send_rows(send_ref, image_rows(nb_ref, h_ref, dir_ref))


def later_kernel(nb_ref, h_ref, res_in, dir_in, sol_in, image_ref, send_ref, res_ref, dir_ref,
                 sol_ref):
    res, direction, sol = step(image_ref[...], res_in[...], dir_in[...], sol_in[...])
    res_ref[...] = res
    dir_ref[...] = direction
    sol_ref[...] = sol
    send_rows(send_ref, image_rows(nb_ref, h_ref, dir_ref))


def final_kernel(nb_ref, h_ref, res_in, dir_in, sol_in, image_ref, send_ref, dir_ref, stats_ref,
                 own_ref, sol_ref):
    res, direction, sol = step(image_ref[...], res_in[...], dir_in[...], sol_in[...])
    dir_ref[...] = direction
    sol_ref[...] = sol
    for at, vec in enumerate((res * res, sol, direction)):
        stats_ref[at] = pair_sums(vec)
    bpd = h_ref.shape[0] // len(STEPS)
    for own in range(bpd):
        mine = nb_ref[own * len(STEPS) + SELF]
        for k in range(2):
            own_ref[pl.ds(2 * own + k, 1), :] = sol_ref[pl.ds(2 * mine + k, 1), :]
            own_ref[pl.ds(2 * (bpd + own) + k, 1), :] = dir_ref[pl.ds(2 * mine + k, 1), :]
    send_rows(send_ref, image_rows(nb_ref, h_ref, dir_ref))


def last_kernel(dir_ref, stats_ref, own_ref, image_ref, out_ref):
    alpha = stats_ref[0] / pair_sums(dir_ref[...] * image_ref[...])
    totals = stats_ref[1] + alpha * stats_ref[2]
    ratio = totals[0:1] / totals[1:2]
    bpd = out_ref.shape[0]
    for own in range(bpd):
        first, second = [
            own_ref[pl.ds(2 * own + k, 1), :]
            + alpha[k : k + 1] * own_ref[pl.ds(2 * (bpd + own) + k, 1), :]
            for k in range(2)
        ]
        out_ref[pl.ds(own, 1), :] = first - ratio * second


def keep(*arrays):
    return [pltpu.with_memory_space_constraint(a, pltpu.VMEM) for a in arrays]


def spread(buf):
    rows = buf.reshape(-1, BLOCK)
    return lax.all_to_all(rows, AXES, 0, 0, tiled=True)


def per_device(offsets, cells, types, mask, chi_table, eta_table, gamma_table):
    n_row = lax.axis_size("row")
    n_col = lax.axis_size("col")
    n_dev = n_row * n_col
    me = lax.axis_index("row") * n_col + lax.axis_index("col")
    bpd = types.shape[0] // BLOCK
    n_blk = n_dev * bpd
    n_pair = bpd * len(STEPS)
    grid = jnp.array([n_row, n_col * bpd // GRID_Z, GRID_Z], jnp.int32)[:, None]

    mine = lax.dynamic_slice_in_dim(cells, me * bpd, bpd, axis=1)
    moves = jnp.array(STEPS, jnp.int32).T
    near = ((mine[:, :, None] + moves[:, None, :] + grid[:, :, None]) % grid[:, :, None])
    found = jnp.all(near.reshape(3, n_pair, 1) == cells[:, None, :], axis=0)
    nb = jnp.sum(jnp.where(found, jnp.arange(n_blk, dtype=jnp.int32)[None], 0), axis=1)

    smem = pl.BlockSpec(memory_space=pltpu.SMEM)
    vmem = pl.BlockSpec(memory_space=pltpu.VMEM)
    params = pltpu.CompilerParams(vmem_limit_bytes=24 * 2**20)
    n_vec = 2 * n_blk
    full = pltpu.VMEM((n_vec, BLOCK), F32)
    send = pltpu.VMEM((n_vec // 8, 8, BLOCK), F32)
    (geo,) = pl.pallas_call(
        pack_kernel,
        out_shape=(pltpu.VMEM((4 * n_blk // 8, 8, BLOCK), F32),),
        in_specs=[pl.BlockSpec(memory_space=pltpu.HBM)] * 2,
        out_specs=(vmem,),
        scratch_shapes=[
            pltpu.VMEM(offsets.shape, F32),
            pltpu.VMEM((bpd, BLOCK), jnp.int32),
            pltpu.SemaphoreType.DMA((2,)),
        ],
        compiler_params=params,
        name="pack",
    )(*[
        pltpu.with_memory_space_constraint(a, pltpu.HBM)
        for a in (offsets, types.reshape(bpd, BLOCK))
    ])
    geo = spread(geo)
    tables = jnp.concatenate([chi_table, eta_table, gamma_table])
    matrix, image, rhs = pl.pallas_call(
        build_kernel,
        out_shape=(pltpu.VMEM((n_pair, BLOCK, BLOCK), F32), send, full),
        in_specs=[smem] * 2 + [vmem],
        out_specs=(vmem,) * 3,
        scratch_shapes=[
            pltpu.VMEM((n_blk, BLOCK), F32),
            pltpu.VMEM((4, BLOCK, BLOCK), F32),
            pltpu.VMEM((2, BLOCK, BLOCK), F32),
        ],
        compiler_params=params,
        name="build",
    )(nb, tables, *keep(geo))
    image = spread(image)
    image, res, direction, sol = pl.pallas_call(
        first_kernel,
        out_shape=(send, full, full, full),
        in_specs=[smem] + [vmem] * 3,
        out_specs=(vmem,) * 4,
        compiler_params=params,
        name="first",
    )(nb, *keep(matrix, rhs, image))
    image = spread(image)
    for _ in range(ITERS - 3):
        image, res, direction, sol = pl.pallas_call(
            later_kernel,
            out_shape=(send, full, full, full),
            in_specs=[smem] + [vmem] * 5,
            out_specs=(vmem,) * 4,
            compiler_params=params,
            name="later",
        )(nb, *keep(matrix, res, direction, sol, image))
        image = spread(image)
    image, direction, stats, own = pl.pallas_call(
        final_kernel,
        out_shape=(
            send,
            full,
            pltpu.VMEM((3, 8, BLOCK), F32),
            pltpu.VMEM((4 * bpd, BLOCK), F32),
        ),
        in_specs=[smem] + [vmem] * 5,
        out_specs=(vmem,) * 4,
        scratch_shapes=[pltpu.VMEM((n_vec, BLOCK), F32)],
        compiler_params=params,
        name="final",
    )(nb, *keep(matrix, res, direction, sol, image))
    out = pl.pallas_call(
        last_kernel,
        out_shape=jax.ShapeDtypeStruct((bpd, BLOCK), F32),
        in_specs=[vmem] * 4,
        out_specs=vmem,
        compiler_params=params,
        name="last",
    )(*keep(direction, stats, own, spread(image)))
    return out.reshape(bpd * BLOCK)


def solution(mesh):
    placed = (
        P(None, AXES),
        P(),
        P(AXES),
        P(None, "col", "row", None),
        P(),
        P(),
        P(),
    )
    return jax.shard_map(
        per_device, mesh=mesh, in_specs=placed, out_specs=P(AXES), check_vma=False
    )
```

```python
import itertools
import jax
import jax.numpy as jnp
from jax import lax
from jax.experimental import pallas as pl
from jax.experimental.pallas import tpu as pltpu
from jax.sharding import PartitionSpec as P

BLOCK = 128
GRID_Z = 4
ITERS = 3

coulomb = 14.4
cutoff = 10.0
cell_side = 11.0
unit = (20.0 * coulomb / cutoff**7) ** (1.0 / 6.0)
reach = unit * cutoff
STEPS = tuple(itertools.product((-1, 0, 1), repeat=3))
SELF = STEPS.index((0, 0, 0))
PLANE = len(STEPS) // 3
AXES = ("row", "col")
F32 = jnp.float32


def column(row):
    return jnp.transpose(jnp.broadcast_to(row, (BLOCK, BLOCK)))


def lane_sums(acc):
    return jnp.sum(jnp.transpose(acc), axis=0, keepdims=True)


def pair_sums(vec):
    part = jnp.sum(vec.reshape(-1, 8, BLOCK), axis=0)
    part = jnp.broadcast_to(jnp.sum(part, axis=1, keepdims=True), (8, BLOCK))
    part = part + pltpu.roll(part, 4, 0)
    return part + pltpu.roll(part, 2, 0)


def scale(vec, factor):
    return (vec.reshape(-1, 8, BLOCK) * factor[None]).reshape(vec.shape)


def send_rows(out_ref, rows):
    own = jnp.concatenate(rows, axis=0)
    own = jnp.concatenate([own] * (8 // own.shape[0]), axis=0)
    out_ref[...] = jnp.broadcast_to(own[None], out_ref.shape)


def by_type(kinds, table_ref, which):
    n_kind = table_ref.shape[0] // 3
    out = jnp.full(kinds.shape, table_ref[which * n_kind], F32)
    for kind in range(1, n_kind):
        out = jnp.where(kinds == float(kind), table_ref[which * n_kind + kind], out)
    return out


def pack_kernel(offsets_in, types_in, send_ref, offsets_ref, types_ref, sems):
    copies = [
        pltpu.make_async_copy(offsets_in, offsets_ref, sems.at[0]),
        pltpu.make_async_copy(types_in, types_ref, sems.at[1]),
    ]
    for copy in copies:
        copy.start()
    for copy in copies:
        copy.wait()
    rows = []
    for own in range(types_ref.shape[0]):
        at = pl.ds(own * BLOCK, BLOCK)
        rows.append(offsets_ref[:, at])
        rows.append(types_ref[pl.ds(own, 1), :].astype(F32))
    send_rows(send_ref, rows)


def build_kernel(nb_ref, table_ref, geo_ref, h_ref, send_ref, rhs_ref,
                 shield_ref, tgt_ref, acc_ref):
    n_blk = shield_ref.shape[0]
    bpd = h_ref.shape[0] // len(STEPS)
    kinds = geo_ref[pl.ds(3, n_blk, stride=4), :]
    gamma = by_type(kinds, table_ref, 2)
    shield_ref[...] = unit**1.5 / (gamma * jnp.sqrt(gamma))
    rhs_ref[pl.ds(0, n_blk, stride=2), :] = -by_type(kinds, table_ref, 0)
    rhs_ref[pl.ds(1, n_blk, stride=2), :] = jnp.full((n_blk, BLOCK), -1.0, F32)
    rows = []
    for own in range(bpd):
        mine = nb_ref[own * len(STEPS) + SELF]
        for comp in range(3):
            tgt_ref[comp] = column(geo_ref[pl.ds(4 * mine + comp, 1), :] * unit)
        tgt_ref[3] = column(shield_ref[pl.ds(mine, 1), :])
        acc_ref[...] = jnp.zeros(acc_ref.shape, F32)

        def plane(at, move, own=own):
            src, shd, first = [], [], []
            for last in range(PLANE):
                blk = nb_ref[own * len(STEPS) + PLANE * at + last]
                shift = (move,) + tuple(float(s) * (cell_side * unit) for s in STEPS[last][1:])
                src.append([
                    jnp.broadcast_to(
                        geo_ref[pl.ds(4 * blk + comp, 1), :] * unit + shift[comp], (8, BLOCK)
                    )
                    for comp in range(3)
                ])
                shd.append(jnp.broadcast_to(shield_ref[pl.ds(blk, 1), :], (8, BLOCK)))
                first.append(jnp.broadcast_to(rhs_ref[pl.ds(2 * blk, 1), :], (8, BLOCK)))
            for chunk in range(BLOCK // 8):
                at_rows = pl.ds(8 * chunk, 8)
                tgt = [tgt_ref[comp, at_rows, :] for comp in range(4)]
                sums = [None, None]
                for last in range(PLANE):
                    gap = [src[last][comp] - tgt[comp] for comp in range(3)]
                    rsq = gap[0] * gap[0] + gap[1] * gap[1] + gap[2] * gap[2]
                    dist = rsq * lax.rsqrt(jnp.maximum(rsq, 1e-30))
                    left = jnp.maximum(reach - dist, 0.0)
                    sq = left * left
                    poly = ((dist + 0.5 * reach) * dist + 0.2 * reach**2) * dist + 0.05 * reach**3
                    wide = rsq * dist + shd[last] * tgt[3]
                    kern = sq * sq * poly * jnp.exp2(jnp.log2(wide) * (-1.0 / 3.0))
                    h_ref[own * len(STEPS) + PLANE * at + last, at_rows, :] = kern
                    part = kern * first[last]
                    sums = [part, kern] if last == 0 else [sums[0] + part, sums[1] + kern]
                acc_ref[0, at_rows, :] += sums[0]
                acc_ref[1, at_rows, :] -= sums[1]
            return move + cell_side * unit

        lax.fori_loop(0, len(STEPS) // PLANE, plane, jnp.float32(-cell_side * unit))
        here = own * len(STEPS) + SELF
        diag = lax.broadcasted_iota(jnp.int32, (BLOCK, BLOCK), 0) == lax.broadcasted_iota(
            jnp.int32, (BLOCK, BLOCK), 1
        )
        eta = by_type(geo_ref[pl.ds(4 * mine + 3, 1), :], table_ref, 1)
        old = h_ref[here]
        new = jnp.where(diag, eta, old)
        h_ref[here] = new
        for k in range(2):
            fix = (new - old) * rhs_ref[pl.ds(2 * mine + k, 1), :]
            rows.append(lane_sums(acc_ref[k] + fix))
    send_rows(send_ref, rows)


def image_rows(nb_ref, h_ref, dir_ref):
    rows = []
    half = BLOCK // 2
    bpd = h_ref.shape[0] // len(STEPS)
    for own in range(bpd):
        parts = ([], [])
        for at_half in range(2):
            acc = [jnp.zeros((half, BLOCK), F32), jnp.zeros((half, BLOCK), F32)]
            for at in range(len(STEPS)):
                pair = own * len(STEPS) + at
                blk = nb_ref[pair]
                h = h_ref[pair, half * at_half : half * (at_half + 1), :]
                for k in range(2):
                    acc[k] = acc[k] + h * dir_ref[pl.ds(2 * blk + k, 1), :]
            for k in range(2):
                parts[k].append(acc[k])
        for k in range(2):
            rows.append(lane_sums(jnp.concatenate(parts[k], axis=0)))
    return rows


def step(image, res, direction, sol):
    norm = pair_sums(res * res)
    alpha = norm / pair_sums(direction * image)
    res = res - scale(image, alpha)
    ratio = pair_sums(res * res) / norm
    move = scale(direction, alpha)
    sol = move if sol is None else sol + move
    return res, res + scale(direction, ratio), sol


def first_kernel(nb_ref, h_ref, rhs_ref, image_ref, send_ref, res_ref, dir_ref, sol_ref):
    rhs = rhs_ref[...]
    res, direction, sol = step(image_ref[...], rhs, rhs, None)
    res_ref[...] = res
    dir_ref[...] = direction
    sol_ref[...] = sol
    send_rows(send_ref, image_rows(nb_ref, h_ref, dir_ref))


def later_kernel(nb_ref, h_ref, res_in, dir_in, sol_in, image_ref, send_ref, res_ref, dir_ref,
                 sol_ref):
    res, direction, sol = step(image_ref[...], res_in[...], dir_in[...], sol_in[...])
    res_ref[...] = res
    dir_ref[...] = direction
    sol_ref[...] = sol
    send_rows(send_ref, image_rows(nb_ref, h_ref, dir_ref))


def final_kernel(nb_ref, h_ref, res_in, dir_in, sol_in, image_ref, send_ref, dir_ref, stats_ref,
                 own_ref, sol_ref):
    res, direction, sol = step(image_ref[...], res_in[...], dir_in[...], sol_in[...])
    dir_ref[...] = direction
    sol_ref[...] = sol
    for at, vec in enumerate((res * res, sol, direction)):
        stats_ref[at] = pair_sums(vec)
    bpd = h_ref.shape[0] // len(STEPS)
    for own in range(bpd):
        mine = nb_ref[own * len(STEPS) + SELF]
        for k in range(2):
            own_ref[pl.ds(2 * own + k, 1), :] = sol_ref[pl.ds(2 * mine + k, 1), :]
            own_ref[pl.ds(2 * (bpd + own) + k, 1), :] = dir_ref[pl.ds(2 * mine + k, 1), :]
    send_rows(send_ref, image_rows(nb_ref, h_ref, dir_ref))


def last_kernel(dir_ref, stats_ref, own_ref, image_ref, out_ref):
    alpha = stats_ref[0] / pair_sums(dir_ref[...] * image_ref[...])
    totals = stats_ref[1] + alpha * stats_ref[2]
    ratio = totals[0:1] / totals[1:2]
    bpd = out_ref.shape[0]
    for own in range(bpd):
        first, second = [
            own_ref[pl.ds(2 * own + k, 1), :]
            + alpha[k : k + 1] * own_ref[pl.ds(2 * (bpd + own) + k, 1), :]
            for k in range(2)
        ]
        out_ref[pl.ds(own, 1), :] = first - ratio * second


def keep(*arrays):
    return [pltpu.with_memory_space_constraint(a, pltpu.VMEM) for a in arrays]


def spread(buf):
    rows = buf.reshape(-1, BLOCK)
    return lax.all_to_all(rows, AXES, 0, 0, tiled=True)


def per_device(offsets, cells, types, mask, chi_table, eta_table, gamma_table):
    n_row = lax.axis_size("row")
    n_col = lax.axis_size("col")
    n_dev = n_row * n_col
    me = lax.axis_index("row") * n_col + lax.axis_index("col")
    bpd = types.shape[0] // BLOCK
    n_blk = n_dev * bpd
    n_pair = bpd * len(STEPS)
    grid = jnp.array([n_row, n_col * bpd // GRID_Z, GRID_Z], jnp.int32)[:, None]

    mine = lax.dynamic_slice_in_dim(cells, me * bpd, bpd, axis=1)
    moves = jnp.array(STEPS, jnp.int32).T
    near = ((mine[:, :, None] + moves[:, None, :] + grid[:, :, None]) % grid[:, :, None])
    found = jnp.all(near.reshape(3, n_pair, 1) == cells[:, None, :], axis=0)
    nb = jnp.sum(jnp.where(found, jnp.arange(n_blk, dtype=jnp.int32)[None], 0), axis=1)

    smem = pl.BlockSpec(memory_space=pltpu.SMEM)
    vmem = pl.BlockSpec(memory_space=pltpu.VMEM)
    params = pltpu.CompilerParams(vmem_limit_bytes=24 * 2**20)
    n_vec = 2 * n_blk
    full = pltpu.VMEM((n_vec, BLOCK), F32)
    send = pltpu.VMEM((n_vec // 8, 8, BLOCK), F32)
    (geo,) = pl.pallas_call(
        pack_kernel,
        out_shape=(pltpu.VMEM((4 * n_blk // 8, 8, BLOCK), F32),),
        in_specs=[pl.BlockSpec(memory_space=pltpu.HBM)] * 2,
        out_specs=(vmem,),
        scratch_shapes=[
            pltpu.VMEM(offsets.shape, F32),
            pltpu.VMEM((bpd, BLOCK), jnp.int32),
            pltpu.SemaphoreType.DMA((2,)),
        ],
        compiler_params=params,
        name="pack",
    )(*[
        pltpu.with_memory_space_constraint(a, pltpu.HBM)
        for a in (offsets, types.reshape(bpd, BLOCK))
    ])
    geo = spread(geo)
    tables = jnp.concatenate([chi_table, eta_table, gamma_table])
    matrix, image, rhs = pl.pallas_call(
        build_kernel,
        out_shape=(pltpu.VMEM((n_pair, BLOCK, BLOCK), F32), send, full),
        in_specs=[smem] * 2 + [vmem],
        out_specs=(vmem,) * 3,
        scratch_shapes=[
            pltpu.VMEM((n_blk, BLOCK), F32),
            pltpu.VMEM((4, BLOCK, BLOCK), F32),
            pltpu.VMEM((2, BLOCK, BLOCK), F32),
        ],
        compiler_params=params,
        name="build",
    )(nb, tables, *keep(geo))
    image = spread(image)
    image, res, direction, sol = pl.pallas_call(
        first_kernel,
        out_shape=(send, full, full, full),
        in_specs=[smem] + [vmem] * 3,
        out_specs=(vmem,) * 4,
        compiler_params=params,
        name="first",
    )(nb, *keep(matrix, rhs, image))
    image = spread(image)
    for _ in range(ITERS - 3):
        image, res, direction, sol = pl.pallas_call(
            later_kernel,
            out_shape=(send, full, full, full),
            in_specs=[smem] + [vmem] * 5,
            out_specs=(vmem,) * 4,
            compiler_params=params,
            name="later",
        )(nb, *keep(matrix, res, direction, sol, image))
        image = spread(image)
    image, direction, stats, own = pl.pallas_call(
        final_kernel,
        out_shape=(
            send,
            full,
            pltpu.VMEM((3, 8, BLOCK), F32),
            pltpu.VMEM((4 * bpd, BLOCK), F32),
        ),
        in_specs=[smem] + [vmem] * 5,
        out_specs=(vmem,) * 4,
        scratch_shapes=[pltpu.VMEM((n_vec, BLOCK), F32)],
        compiler_params=params,
        name="final",
    )(nb, *keep(matrix, res, direction, sol, image))
    out = pl.pallas_call(
        last_kernel,
        out_shape=jax.ShapeDtypeStruct((bpd, BLOCK), F32),
        in_specs=[vmem] * 4,
        out_specs=vmem,
        compiler_params=params,
        name="last",
    )(*keep(direction, stats, own, spread(image)))
    return out.reshape(bpd * BLOCK)


def solution(mesh):
    placed = (
        P(None, AXES),
        P(),
        P(AXES),
        P(None, "col", "row", None),
        P(),
        P(),
        P(),
    )
    return jax.shard_map(
        per_device, mesh=mesh, in_specs=placed, out_specs=P(AXES), check_vma=False
    )
```

```python
import itertools
import jax
import jax.numpy as jnp
from jax import lax
from jax.experimental import pallas as pl
from jax.experimental.pallas import tpu as pltpu
from jax.sharding import PartitionSpec as P

BLOCK = 128
GRID_Z = 4
ITERS = 3

coulomb = 14.4
cutoff = 10.0
cell_side = 11.0
unit = (20.0 * coulomb / cutoff**7) ** (1.0 / 6.0)
reach = unit * cutoff
STEPS = tuple(itertools.product((-1, 0, 1), repeat=3))
SELF = STEPS.index((0, 0, 0))
PLANE = len(STEPS) // 3
AXES = ("row", "col")
F32 = jnp.float32


def column(row):
    return jnp.transpose(jnp.broadcast_to(row, (BLOCK, BLOCK)))


def lane_sums(acc):
    return jnp.sum(jnp.transpose(acc), axis=0, keepdims=True)


def pair_sums(vec):
    part = jnp.sum(vec.reshape(-1, 8, BLOCK), axis=0)
    part = jnp.broadcast_to(jnp.sum(part, axis=1, keepdims=True), (8, BLOCK))
    part = part + pltpu.roll(part, 4, 0)
    return part + pltpu.roll(part, 2, 0)


def scale(vec, factor):
    return (vec.reshape(-1, 8, BLOCK) * factor[None]).reshape(vec.shape)


def send_rows(out_ref, rows):
    own = jnp.concatenate(rows, axis=0)
    own = jnp.concatenate([own] * (8 // own.shape[0]), axis=0)
    out_ref[...] = jnp.broadcast_to(own[None], out_ref.shape)


def by_type(kinds, table_ref, which):
    n_kind = table_ref.shape[0] // 3
    out = jnp.full(kinds.shape, table_ref[which * n_kind], F32)
    for kind in range(1, n_kind):
        out = jnp.where(kinds == float(kind), table_ref[which * n_kind + kind], out)
    return out


def pack_kernel(offsets_in, types_in, send_ref, offsets_ref, types_ref, sems):
    copies = [
        pltpu.make_async_copy(offsets_in, offsets_ref, sems.at[0]),
        pltpu.make_async_copy(types_in, types_ref, sems.at[1]),
    ]
    for copy in copies:
        copy.start()
    for copy in copies:
        copy.wait()
    rows = []
    for own in range(types_ref.shape[0]):
        at = pl.ds(own * BLOCK, BLOCK)
        rows.append(offsets_ref[:, at])
        rows.append(types_ref[pl.ds(own, 1), :].astype(F32))
    send_rows(send_ref, rows)


def build_kernel(nb_ref, table_ref, geo_ref, h_ref, send_ref, rhs_ref,
                 shield_ref, tgt_ref, acc_ref):
    n_blk = shield_ref.shape[0]
    bpd = h_ref.shape[0] // len(STEPS)
    kinds = geo_ref[pl.ds(3, n_blk, stride=4), :]
    gamma = by_type(kinds, table_ref, 2)
    shield_ref[...] = unit**1.5 / (gamma * jnp.sqrt(gamma))
    rhs_ref[pl.ds(0, n_blk, stride=2), :] = -by_type(kinds, table_ref, 0)
    rhs_ref[pl.ds(1, n_blk, stride=2), :] = jnp.full((n_blk, BLOCK), -1.0, F32)
    rows = []
    for own in range(bpd):
        mine = nb_ref[own * len(STEPS) + SELF]
        for comp in range(3):
            tgt_ref[comp] = column(geo_ref[pl.ds(4 * mine + comp, 1), :] * unit)
        tgt_ref[3] = column(shield_ref[pl.ds(mine, 1), :])
        acc_ref[...] = jnp.zeros(acc_ref.shape, F32)

        def plane(at, move, own=own):
            src, shd, first = [], [], []
            for last in range(PLANE):
                blk = nb_ref[own * len(STEPS) + PLANE * at + last]
                shift = (move,) + tuple(float(s) * (cell_side * unit) for s in STEPS[last][1:])
                src.append([
                    jnp.broadcast_to(
                        geo_ref[pl.ds(4 * blk + comp, 1), :] * unit + shift[comp], (8, BLOCK)
                    )
                    for comp in range(3)
                ])
                shd.append(jnp.broadcast_to(shield_ref[pl.ds(blk, 1), :], (8, BLOCK)))
                first.append(jnp.broadcast_to(rhs_ref[pl.ds(2 * blk, 1), :], (8, BLOCK)))
            for chunk in range(BLOCK // 8):
                at_rows = pl.ds(8 * chunk, 8)
                tgt = [tgt_ref[comp, at_rows, :] for comp in range(4)]
                sums = [None, None]
                for last in range(PLANE):
                    gap = [src[last][comp] - tgt[comp] for comp in range(3)]
                    rsq = gap[0] * gap[0] + gap[1] * gap[1] + gap[2] * gap[2]
                    dist = rsq * lax.rsqrt(jnp.maximum(rsq, 1e-30))
                    left = jnp.maximum(reach - dist, 0.0)
                    sq = left * left
                    poly = ((dist + 0.5 * reach) * dist + 0.2 * reach**2) * dist + 0.05 * reach**3
                    wide = rsq * dist + shd[last] * tgt[3]
                    kern = sq * sq * poly * jnp.exp2(jnp.log2(wide) * (-1.0 / 3.0))
                    h_ref[own * len(STEPS) + PLANE * at + last, at_rows, :] = kern
                    part = kern * first[last]
                    sums = [part, kern] if last == 0 else [sums[0] + part, sums[1] + kern]
                acc_ref[0, at_rows, :] += sums[0]
                acc_ref[1, at_rows, :] -= sums[1]
            return move + cell_side * unit

        lax.fori_loop(0, len(STEPS) // PLANE, plane, jnp.float32(-cell_side * unit))
        here = own * len(STEPS) + SELF
        diag = lax.broadcasted_iota(jnp.int32, (BLOCK, BLOCK), 0) == lax.broadcasted_iota(
            jnp.int32, (BLOCK, BLOCK), 1
        )
        eta = by_type(geo_ref[pl.ds(4 * mine + 3, 1), :], table_ref, 1)
        old = h_ref[here]
        new = jnp.where(diag, eta, old)
        h_ref[here] = new
        for k in range(2):
            fix = (new - old) * rhs_ref[pl.ds(2 * mine + k, 1), :]
            rows.append(lane_sums(acc_ref[k] + fix))
    send_rows(send_ref, rows)


def image_rows(nb_ref, h_ref, dir_ref):
    rows = []
    half = BLOCK
    bpd = h_ref.shape[0] // len(STEPS)
    for own in range(bpd):
        parts = ([], [])
        for at_half in range(BLOCK // half):
            acc = [jnp.zeros((half, BLOCK), F32), jnp.zeros((half, BLOCK), F32)]
            for at in range(len(STEPS)):
                pair = own * len(STEPS) + at
                blk = nb_ref[pair]
                h = h_ref[pair, half * at_half : half * (at_half + 1), :]
                for k in range(2):
                    acc[k] = acc[k] + h * dir_ref[pl.ds(2 * blk + k, 1), :]
            for k in range(2):
                parts[k].append(acc[k])
        for k in range(2):
            rows.append(lane_sums(jnp.concatenate(parts[k], axis=0)))
    return rows


def step(image, res, direction, sol):
    norm = pair_sums(res * res)
    alpha = norm / pair_sums(direction * image)
    res = res - scale(image, alpha)
    ratio = pair_sums(res * res) / norm
    move = scale(direction, alpha)
    sol = move if sol is None else sol + move
    return res, res + scale(direction, ratio), sol


def first_kernel(nb_ref, h_ref, rhs_ref, image_ref, send_ref, res_ref, dir_ref, sol_ref):
    rhs = rhs_ref[...]
    res, direction, sol = step(image_ref[...], rhs, rhs, None)
    res_ref[...] = res
    dir_ref[...] = direction
    sol_ref[...] = sol
    send_rows(send_ref, image_rows(nb_ref, h_ref, dir_ref))


def later_kernel(nb_ref, h_ref, res_in, dir_in, sol_in, image_ref, send_ref, res_ref, dir_ref,
                 sol_ref):
    res, direction, sol = step(image_ref[...], res_in[...], dir_in[...], sol_in[...])
    res_ref[...] = res
    dir_ref[...] = direction
    sol_ref[...] = sol
    send_rows(send_ref, image_rows(nb_ref, h_ref, dir_ref))


def final_kernel(nb_ref, h_ref, res_in, dir_in, sol_in, image_ref, send_ref, dir_ref, stats_ref,
                 own_ref, sol_ref):
    res, direction, sol = step(image_ref[...], res_in[...], dir_in[...], sol_in[...])
    dir_ref[...] = direction
    sol_ref[...] = sol
    for at, vec in enumerate((res * res, sol, direction)):
        stats_ref[at] = pair_sums(vec)
    bpd = h_ref.shape[0] // len(STEPS)
    for own in range(bpd):
        mine = nb_ref[own * len(STEPS) + SELF]
        for k in range(2):
            own_ref[pl.ds(2 * own + k, 1), :] = sol_ref[pl.ds(2 * mine + k, 1), :]
            own_ref[pl.ds(2 * (bpd + own) + k, 1), :] = dir_ref[pl.ds(2 * mine + k, 1), :]
    send_rows(send_ref, image_rows(nb_ref, h_ref, dir_ref))


def last_kernel(dir_ref, stats_ref, own_ref, image_ref, out_ref):
    alpha = stats_ref[0] / pair_sums(dir_ref[...] * image_ref[...])
    totals = stats_ref[1] + alpha * stats_ref[2]
    ratio = totals[0:1] / totals[1:2]
    bpd = out_ref.shape[0]
    for own in range(bpd):
        first, second = [
            own_ref[pl.ds(2 * own + k, 1), :]
            + alpha[k : k + 1] * own_ref[pl.ds(2 * (bpd + own) + k, 1), :]
            for k in range(2)
        ]
        out_ref[pl.ds(own, 1), :] = first - ratio * second


def keep(*arrays):
    return [pltpu.with_memory_space_constraint(a, pltpu.VMEM) for a in arrays]


def spread(buf):
    rows = buf.reshape(-1, BLOCK)
    return lax.all_to_all(rows, AXES, 0, 0, tiled=True)


def per_device(offsets, cells, types, mask, chi_table, eta_table, gamma_table):
    n_row = lax.axis_size("row")
    n_col = lax.axis_size("col")
    n_dev = n_row * n_col
    me = lax.axis_index("row") * n_col + lax.axis_index("col")
    bpd = types.shape[0] // BLOCK
    n_blk = n_dev * bpd
    n_pair = bpd * len(STEPS)
    grid = jnp.array([n_row, n_col * bpd // GRID_Z, GRID_Z], jnp.int32)[:, None]

    mine = lax.dynamic_slice_in_dim(cells, me * bpd, bpd, axis=1)
    moves = jnp.array(STEPS, jnp.int32).T
    near = ((mine[:, :, None] + moves[:, None, :] + grid[:, :, None]) % grid[:, :, None])
    found = jnp.all(near.reshape(3, n_pair, 1) == cells[:, None, :], axis=0)
    nb = jnp.sum(jnp.where(found, jnp.arange(n_blk, dtype=jnp.int32)[None], 0), axis=1)

    smem = pl.BlockSpec(memory_space=pltpu.SMEM)
    vmem = pl.BlockSpec(memory_space=pltpu.VMEM)
    params = pltpu.CompilerParams(vmem_limit_bytes=24 * 2**20)
    n_vec = 2 * n_blk
    full = pltpu.VMEM((n_vec, BLOCK), F32)
    send = pltpu.VMEM((n_vec // 8, 8, BLOCK), F32)
    (geo,) = pl.pallas_call(
        pack_kernel,
        out_shape=(pltpu.VMEM((4 * n_blk // 8, 8, BLOCK), F32),),
        in_specs=[pl.BlockSpec(memory_space=pltpu.HBM)] * 2,
        out_specs=(vmem,),
        scratch_shapes=[
            pltpu.VMEM(offsets.shape, F32),
            pltpu.VMEM((bpd, BLOCK), jnp.int32),
            pltpu.SemaphoreType.DMA((2,)),
        ],
        compiler_params=params,
        name="pack",
    )(*[
        pltpu.with_memory_space_constraint(a, pltpu.HBM)
        for a in (offsets, types.reshape(bpd, BLOCK))
    ])
    geo = spread(geo)
    tables = jnp.concatenate([chi_table, eta_table, gamma_table])
    matrix, image, rhs = pl.pallas_call(
        build_kernel,
        out_shape=(pltpu.VMEM((n_pair, BLOCK, BLOCK), F32), send, full),
        in_specs=[smem] * 2 + [vmem],
        out_specs=(vmem,) * 3,
        scratch_shapes=[
            pltpu.VMEM((n_blk, BLOCK), F32),
            pltpu.VMEM((4, BLOCK, BLOCK), F32),
            pltpu.VMEM((2, BLOCK, BLOCK), F32),
        ],
        compiler_params=params,
        name="build",
    )(nb, tables, *keep(geo))
    image = spread(image)
    image, res, direction, sol = pl.pallas_call(
        first_kernel,
        out_shape=(send, full, full, full),
        in_specs=[smem] + [vmem] * 3,
        out_specs=(vmem,) * 4,
        compiler_params=params,
        name="first",
    )(nb, *keep(matrix, rhs, image))
    image = spread(image)
    for _ in range(ITERS - 3):
        image, res, direction, sol = pl.pallas_call(
            later_kernel,
            out_shape=(send, full, full, full),
            in_specs=[smem] + [vmem] * 5,
            out_specs=(vmem,) * 4,
            compiler_params=params,
            name="later",
        )(nb, *keep(matrix, res, direction, sol, image))
        image = spread(image)
    image, direction, stats, own = pl.pallas_call(
        final_kernel,
        out_shape=(
            send,
            full,
            pltpu.VMEM((3, 8, BLOCK), F32),
            pltpu.VMEM((4 * bpd, BLOCK), F32),
        ),
        in_specs=[smem] + [vmem] * 5,
        out_specs=(vmem,) * 4,
        scratch_shapes=[pltpu.VMEM((n_vec, BLOCK), F32)],
        compiler_params=params,
        name="final",
    )(nb, *keep(matrix, res, direction, sol, image))
    out = pl.pallas_call(
        last_kernel,
        out_shape=jax.ShapeDtypeStruct((bpd, BLOCK), F32),
        in_specs=[vmem] * 4,
        out_specs=vmem,
        compiler_params=params,
        name="last",
    )(*keep(direction, stats, own, spread(image)))
    return out.reshape(bpd * BLOCK)


def solution(mesh):
    placed = (
        P(None, AXES),
        P(),
        P(AXES),
        P(None, "col", "row", None),
        P(),
        P(),
        P(),
    )
    return jax.shard_map(
        per_device, mesh=mesh, in_specs=placed, out_specs=P(AXES), check_vma=False
    )
```
